32 devices in a mesh: seq: 8 (over z, y), rep: 4 (over x, core).
Axes of the slice: x: 2, y: 2, z: 4, core: 2. Of those that a mesh axis runs over, the one named last changes fastest.
Arguments:
- head_out: bfloat16 [4, 4096, 4096], P('rep', 'seq'), may hold values from -6 to 6
- grad_out: bfloat16 [4, 4096, 3584], P('rep', 'seq'), may hold values from -6 to 6
- hash_codes: int32 [4, 16, 3584], P('rep'), may hold values from 0 to 511
- loss_mask: int32 [4096], P('seq'), may hold values 0 or 1
- query_ids: int32 [64], replicated, may hold values from 0 to 4095
Outputs:
- attribution: float32 [4096, 64], P(('seq', 'rep'))
The draws below stay inside these ranges and needn't reach their ends.
All inputs are finite; a program needn't handle non-finite values. No bound on the sum of `loss_mask` on one device may be relied on, other than what follows from the above.
Results may differ from the reference program's by a relative error of at most 0.0025.
Values may be sent and summed in bfloat16 or wider, within the bound.
A program may use at most 64 MiB of HBM per device.

```python
import math
import jax
import jax.numpy as jnp
from jax import lax

D = 3584
HEADS = 16
HEAD_DIM = 256
QUERIES = 64
TOKENS = 4096
LAYERS = 4


def set_ends(array, key, low, high):
    place = [jax.random.randint(jax.random.fold_in(key, axis), (), 0, length) for axis, length in enumerate(array.shape)]
    widest = array.shape.index(max(array.shape))
    neighbour = place[:widest] + [(place[widest] + 1) % array.shape[widest]] + place[widest + 1:]
    return array.at[tuple(place)].set(low).at[tuple(neighbour)].set(high)


def shard_levels(own_key, dims, pieces, smallest, high):
    loudness, own = 1.0, jax.random.fold_in(own_key, 6)
    for position, shards_of in pieces:
        heights = jnp.exp(jax.random.uniform(jax.random.fold_in(own, position), (shards_of,), jnp.float32, smallest / len(pieces), high / len(pieces)))
        loudness = loudness * jnp.repeat(heights, dims[position] // shards_of).reshape([-1 if axis == position else 1 for axis in range(len(dims))])
    return loudness


def noise(rng, shape, scale, most, split=(), kind=jnp.bfloat16):
    loudness = shard_levels(rng, shape, split, -0.22, 0.18) if split else 1.0
    drawn = jax.random.normal(rng, shape, jnp.float32) * scale * loudness
    return jnp.minimum(jnp.maximum(drawn, -most), most).astype(kind)


def setup_inputs(seed: int = 0) -> dict:
    key_list = jax.random.split(jax.random.key(seed), 6)
    head_out = noise(key_list[0], (LAYERS, TOKENS, HEADS * HEAD_DIM), 1.0, 6.0, ((0, 4), (1, 8)))
    grad_out = noise(key_list[1], (LAYERS, TOKENS, D), 1.0, 6.0, ((0, 4), (1, 8)))
    hash_codes = set_ends(jax.random.randint(key_list[2], (LAYERS, HEADS, D), 0, 2 * HEAD_DIM), jax.random.fold_in(key_list[2], 1), 0, (2 * HEAD_DIM) - 1).astype(jnp.int32)
    loss_mask = set_ends((jax.random.randint(key_list[3], (TOKENS,), 0, 4) < 3).astype(jnp.int32), jax.random.fold_in(key_list[3], 1), 0, 1)
    query_ids = set_ends(jax.random.randint(key_list[4], (QUERIES,), 0, TOKENS), jax.random.fold_in(key_list[4], 1), 0, TOKENS - 1).astype(jnp.int32)
    return dict(head_out=head_out, grad_out=grad_out, hash_codes=hash_codes, loss_mask=loss_mask, query_ids=query_ids)


ridge_shift = 0.25
norm_floor = 1e-06

def sketch_head(out_cols, grad_t, head_codes):
    sketch_width = out_cols.shape[1]
    bucket = head_codes % sketch_width
    sign_flip = (1 - 2 * (head_codes // sketch_width)).astype(jnp.float32)
    counted = jax.ops.segment_sum(grad_t * sign_flip[:, None], bucket, num_segments=sketch_width)
    sketch_scale = math.sqrt(sketch_width / grad_t.shape[0])
    return (out_cols.astype(jnp.float32) * counted.T * sketch_scale).astype(jnp.bfloat16)

def head_scores(sketch, mask_bf, token_count, query_ids):
    sketch_width = sketch.shape[1]
    gram_sum = jnp.dot((sketch * mask_bf[:, None]).T.astype(jnp.float32), sketch.astype(jnp.float32), preferred_element_type=jnp.float32)
    gram_sum = gram_sum / token_count + ridge_shift * jnp.eye(sketch_width, dtype=jnp.float32)
    chosen = sketch[query_ids].astype(jnp.float32)
    factor = jnp.linalg.cholesky(gram_sum)
    solved = jax.scipy.linalg.cho_solve((factor, True), chosen.T).astype(jnp.bfloat16)
    return jnp.dot(sketch.astype(jnp.float32), solved.astype(jnp.float32), preferred_element_type=jnp.float32)

def reference(head_out, grad_out, hash_codes, loss_mask, query_ids):
    mask_f = loss_mask.astype(jnp.float32)
    mask_bf = loss_mask.astype(jnp.bfloat16)
    token_count = jnp.sum(mask_f) + jnp.float32(1.0)
    score_sum = jnp.zeros((TOKENS, QUERIES), jnp.float32)
    for layer_index in range(LAYERS):
        grad_t = grad_out[layer_index].astype(jnp.float32).T
        outputs = head_out[layer_index]
        codes = hash_codes[layer_index]

        def add_head(carry, head_index):
            out_cols = lax.dynamic_slice_in_dim(outputs, head_index * HEAD_DIM, HEAD_DIM, 1)
            sketch = sketch_head(out_cols, grad_t, codes[head_index])
            return (carry + head_scores(sketch, mask_bf, token_count, query_ids), None)
        score_sum, _ = lax.scan(add_head, score_sum, jnp.arange(HEADS, dtype=jnp.int32))
    norm_sum = lax.optimization_barrier(jnp.sum(mask_f[:, None] * score_sum * score_sum, 0)) / token_count
    return score_sum / jnp.sqrt(norm_sum + norm_floor)
```

```python
import functools
import math

import jax
import jax.numpy as jnp
from jax import lax
from jax.experimental import pallas as pl
from jax.experimental.pallas import tpu as pltpu
from jax.sharding import PartitionSpec as P

ridge_shift = 0.25
norm_floor = 1e-06
NT = (((1,), (1,)), ((), ()))
TN = (((0,), (0,)), ((), ()))


def exact_dot(a, b, dims=(((1,), (0,)), ((), ()))):
    return lax.dot_general(
        a, b, dims, precision=lax.Precision.HIGHEST, preferred_element_type=jnp.float32
    )


def spd_inverse(mats):
    size = mats[0].shape[0]
    lane = lax.broadcasted_iota(jnp.int32, (1, size), 1)
    row8 = lax.broadcasted_iota(jnp.int32, (8, 1), 0)

    def pivots(_, mats):
        mats = list(mats)
        for k in range(8):
            for i, m in enumerate(mats):
                row, col = m[k : k + 1, :], m[:, k : k + 1]
                inv = 1.0 / row[:, k : k + 1]
                scaled = jnp.where(lane == k, inv, row * inv)
                new = jnp.where(lane == k, 0.0, m) - col * scaled
                top = jnp.where(row8 == k, scaled, new[:8])
                mats[i] = jnp.concatenate([top, new[8:]], axis=0)
        return tuple(
            pltpu.roll(jnp.concatenate([m[8:], m[:8]], axis=0), size - 8, 1) for m in mats
        )

    return lax.fori_loop(0, size // 8, pivots, tuple(mats))


def solve_rows(grams, rows):
    half = grams[0].shape[0] // 2
    inv_a = spd_inverse([g[:half, :half] for g in grams])
    cross = [g[:half, half:] for g in grams]
    w = [exact_dot(ia, b) for ia, b in zip(inv_a, cross)]
    inv_s = spd_inverse(
        [g[half:, half:] - exact_dot(b, wi, TN) for g, b, wi in zip(grams, cross, w)]
    )
    out = []
    for r, ia, wi, si in zip(rows, inv_a, w, inv_s):
        second = exact_dot(r[:, half:] - exact_dot(r[:, :half], wi), si)
        first = exact_dot(r[:, :half], ia) - exact_dot(second, wi, NT)
        out.append(jnp.concatenate([first, second], axis=1))
    return out


def sketch_kernel(scale, grad_ref, out_ref, codes_ref, mask_ref, hits_ref, sk_ref, gram_ref, ch_ref):
    head = pl.program_id(0)
    width = out_ref.shape[1]
    depth = grad_ref.shape[1]
    codes = codes_ref[pl.ds(head, 1), :]
    bucket = (codes % width).astype(jnp.float32).astype(jnp.bfloat16)
    sign = (1 - 2 * (codes // width)).astype(jnp.float32).astype(jnp.bfloat16)
    want = lax.broadcasted_iota(jnp.int32, (width, depth), 0).astype(jnp.float32).astype(jnp.bfloat16)
    table = jnp.where(bucket == want, sign, jnp.bfloat16(0))
    hashed = lax.dot_general(grad_ref[...], table, NT, preferred_element_type=jnp.float32)
    sketch = (out_ref[...].astype(jnp.float32) * hashed * scale).astype(jnp.bfloat16)
    sk_ref[...] = sketch
    gram_ref[0] = lax.dot_general(
        sketch * mask_ref[...], sketch, TN, preferred_element_type=jnp.float32
    )
    ch_ref[0] = jnp.dot(hits_ref[...], sketch, preferred_element_type=jnp.float32)


def sketch_all(outputs, gradient, codes, mask_col, hits):
    heads, depth = codes.shape
    rows, cols = outputs.shape
    width = cols // heads
    queries = hits.shape[0]
    whole = lambda h: (0, 0)
    once = pl.Buffered(1)

    return pl.pallas_call(
        functools.partial(sketch_kernel, math.sqrt(width / depth)),
        grid=(heads,),
        in_specs=[
            pl.BlockSpec((rows, depth), whole, pipeline_mode=once),
            pl.BlockSpec((rows, width), lambda h: (0, h)),
            pl.BlockSpec((heads, depth), whole, pipeline_mode=once),
            pl.BlockSpec((rows, 1), whole, pipeline_mode=once),
            pl.BlockSpec((queries, rows), whole, pipeline_mode=once),
        ],
        out_specs=[
            pl.BlockSpec((rows, width), lambda h: (0, h)),
            pl.BlockSpec((1, width, width), lambda h: (h, 0, 0)),
            pl.BlockSpec((1, queries, width), lambda h: (h, 0, 0)),
        ],
        out_shape=[
            jax.ShapeDtypeStruct((rows, cols), jnp.bfloat16),
            jax.ShapeDtypeStruct((heads, width, width), jnp.float32),
            jax.ShapeDtypeStruct((heads, queries, width), jnp.float32),
        ],
        compiler_params=pltpu.CompilerParams(vmem_limit_bytes=40 << 20),
        cost_estimate=pl.CostEstimate(
            flops=2 * rows * depth * cols, bytes_accessed=4 * rows * cols, transcendentals=0
        ),
        name="sketch",
    )(gradient, outputs, codes, mask_col, hits)


def solve_kernel(count_ref, gram_ref, ch_ref, out_ref):
    width = gram_ref.shape[1]
    diag = lax.broadcasted_iota(jnp.int32, (width, width), 0) == lax.broadcasted_iota(
        jnp.int32, (width, width), 1
    )
    ridge = jnp.where(diag, ridge_shift, 0.0)
    slots = range(gram_ref.shape[0])
    grams = [gram_ref[i] / count_ref[0, 0] + ridge for i in slots]
    for i, solved in enumerate(solve_rows(grams, [ch_ref[i] for i in slots])):
        out_ref[i] = solved.astype(jnp.bfloat16)


def solve_all(count, grams, chosen):
    vmem = pl.BlockSpec(memory_space=pltpu.VMEM)
    return pl.pallas_call(
        solve_kernel,
        in_specs=[pl.BlockSpec(memory_space=pltpu.SMEM), vmem, vmem],
        out_specs=vmem,
        out_shape=jax.ShapeDtypeStruct(chosen.shape, jnp.bfloat16),
        name="solve",
    )(count.reshape(1, 1), grams, chosen)


def on_device(head_out, grad_out, hash_codes, loss_mask, query_ids):
    tok_rows = loss_mask.shape[0]
    out_rows = tok_rows // lax.axis_size("rep")
    local_count = jnp.sum(loss_mask.astype(jnp.float32))
    token_count = lax.psum(local_count, "seq") + 1.0
    first_row = lax.axis_index("seq") * tok_rows
    query_hits = (
        query_ids[:, None] - first_row == jnp.arange(tok_rows, dtype=jnp.int32)[None, :]
    ).astype(jnp.bfloat16)
    sketches, local_grams, local_chosen = sketch_all(
        head_out[0], grad_out[0], hash_codes[0], loss_mask.astype(jnp.bfloat16)[:, None], query_hits
    )
    own_grams = lax.psum_scatter(local_grams, "seq", scatter_dimension=0, tiled=True)
    own_chosen = lax.psum_scatter(local_chosen, "seq", scatter_dimension=0, tiled=True)
    solved = solve_all(token_count, own_grams, own_chosen)
    solved_all = lax.all_gather(solved, "seq", axis=0, tiled=True)
    heads, queries, width = solved_all.shape
    score_sum = jnp.einsum(
        "thk,hqk->tq",
        sketches.reshape(tok_rows, heads, width),
        solved_all,
        preferred_element_type=jnp.float32,
    )
    contrib = lax.psum_scatter(score_sum, "rep", scatter_dimension=0, tiled=True)
    row_start = lax.axis_index("rep") * out_rows
    mask_rows = lax.dynamic_slice_in_dim(loss_mask, row_start, out_rows, 0).astype(jnp.float32)
    partial_value = jnp.sum(mask_rows[:, None] * contrib * contrib, 0)
    norm_sum = lax.psum(partial_value, ("seq", "rep")) / token_count
    return contrib / jnp.sqrt(norm_sum + norm_floor)


def solution(mesh):
    placed = (P("rep", "seq", None), P("rep", "seq", None), P("rep", None, None), P("seq"), P())
    return jax.shard_map(
        on_device, mesh=mesh, in_specs=placed, out_specs=P(("seq", "rep"), None), check_vma=False
    )
```

```python
import functools
import math

import jax
import jax.numpy as jnp
from jax import lax
from jax.experimental import pallas as pl
from jax.experimental.pallas import tpu as pltpu
from jax.sharding import PartitionSpec as P

ridge_shift = 0.25
norm_floor = 1e-06
NT = (((1,), (1,)), ((), ()))
TN = (((0,), (0,)), ((), ()))


def exact_dot(a, b, dims=(((1,), (0,)), ((), ()))):
    return lax.dot_general(
        a, b, dims, precision=lax.Precision.HIGHEST, preferred_element_type=jnp.float32
    )


def spd_inverse(mats):
    size = mats[0].shape[0]
    lane = lax.broadcasted_iota(jnp.int32, (1, size), 1)
    row8 = lax.broadcasted_iota(jnp.int32, (8, 1), 0)

    def pivots(_, mats):
        mats = list(mats)
        for k in range(8):
            for i, m in enumerate(mats):
                row, col = m[k : k + 1, :], m[:, k : k + 1]
                inv = 1.0 / row[:, k : k + 1]
                scaled = jnp.where(lane == k, inv, row * inv)
                new = jnp.where(lane == k, 0.0, m) - col * scaled
                top = jnp.where(row8 == k, scaled, new[:8])
                mats[i] = jnp.concatenate([top, new[8:]], axis=0)
        return tuple(
            pltpu.roll(jnp.concatenate([m[8:], m[:8]], axis=0), size - 8, 1) for m in mats
        )

    return lax.fori_loop(0, size // 8, pivots, tuple(mats))


def solve_rows(blocks, rows):
    half = blocks[0][0].shape[0]
    inv_a = spd_inverse([a for a, _, _ in blocks])
    w = [exact_dot(ia, b) for ia, (_, b, _) in zip(inv_a, blocks)]
    inv_s = spd_inverse([c - exact_dot(b, wi, TN) for (_, b, c), wi in zip(blocks, w)])
    out = []
    for r, ia, wi, si in zip(rows, inv_a, w, inv_s):
        second = exact_dot(r[:, half:] - exact_dot(r[:, :half], wi), si)
        first = exact_dot(r[:, :half], ia) - exact_dot(second, wi, NT)
        out.append(jnp.concatenate([first, second], axis=1))
    return out


def peer_copy(src, dst, send, recv, axis, index):
    return pltpu.make_async_remote_copy(
        src_ref=src,
        dst_ref=dst,
        send_sem=send,
        recv_sem=recv,
        device_id={axis: index},
        device_id_type=pl.DeviceIdType.MESH,
    )


def others(axis, body):
    size, me = lax.axis_size(axis), lax.axis_index(axis)

    def step(s, carry):
        body(lax.rem(me + 1 + s, size))
        return carry

    lax.fori_loop(0, size - 1, step, 0)


def whole_kernel(
    scale,
    own_heads,
    grad_ref,
    cols_ref,
    codes_ref,
    mask_ref,
    ids_ref,
    out_ref,
    sk_ref,
    hits_ref,
    gram_stage,
    gram_in,
    ch_stage,
    ch_in,
    solved_ref,
    score_ref,
    score_in,
    rep_norm,
    seq_norm,
    gram_sems,
    ch_sems,
    solved_sems,
    score_sems,
    rep_sems,
    seq_sems,
):
    n_seq, n_rep = lax.axis_size("seq"), lax.axis_size("rep")
    me, layer = lax.axis_index("seq"), lax.axis_index("rep")
    rows, depth = grad_ref.shape
    width = cols_ref.shape[1] // codes_ref.shape[0]
    half = width // 2
    out_rows = out_ref.shape[0]

    barrier = pltpu.get_barrier_semaphore()
    for axis in ("seq", "rep"):
        others(
            axis,
            lambda peer, axis=axis: pl.semaphore_signal(
                barrier, inc=1, device_id={axis: peer}, device_id_type=pl.DeviceIdType.MESH
            ),
        )

    mask = mask_ref[...]
    count = jnp.sum(mask, axis=0, keepdims=True)
    token = lax.broadcasted_iota(jnp.int32, (ids_ref.shape[0], rows), 1)
    hits_ref[...] = jnp.where(ids_ref[...] - me * rows == token, 1.0, 0.0).astype(jnp.bfloat16)

    def sketch_head(head, gram_to, ch_to):
        codes = codes_ref[pl.ds(head, 1), :]
        flipped = codes >= width
        bucket = jnp.where(flipped, codes - width, codes)
        bucket = bucket.astype(jnp.float32).astype(jnp.bfloat16)
        sign = jnp.where(flipped, -1.0, 1.0).astype(jnp.bfloat16)
        want = lax.broadcasted_iota(jnp.int32, (width, depth), 0)
        want = want.astype(jnp.float32).astype(jnp.bfloat16)
        table = jnp.where(bucket == want, sign, jnp.bfloat16(0))
        hashed = lax.dot_general(grad_ref[...], table, NT, preferred_element_type=jnp.float32)
        span = pl.ds(pl.multiple_of(head * width, width), width)
        sketch = (cols_ref[:, span].astype(jnp.float32) * hashed * scale).astype(jnp.bfloat16)
        sk_ref[:, span] = sketch
        gram = lax.dot_general(
            sketch * mask_ref[...].astype(jnp.bfloat16),
            sketch,
            TN,
            preferred_element_type=jnp.float32,
        )
        gram_to[:half, :width] = gram[:half]
        gram_to[:half, width:] = gram[half:, half:]
        gram_to[half:, :] = jnp.broadcast_to(count, (8, width + half))
        ch_to[...] = jnp.dot(
            hits_ref[...], sketch, preferred_element_type=jnp.float32
        ).astype(jnp.bfloat16)

    def gram_copy(peer, slot, source):
        return peer_copy(
            gram_stage.at[peer, slot],
            gram_in.at[source, slot],
            gram_sems.at[0, peer, slot],
            gram_sems.at[1, source, slot],
            "seq",
            peer,
        )

    def ch_copy(peer, slot, source):
        return peer_copy(
            ch_stage.at[peer, slot],
            ch_in.at[source, slot],
            ch_sems.at[0, peer, slot],
            ch_sems.at[1, source, slot],
            "seq",
            peer,
        )

    pl.semaphore_wait(barrier, n_seq + n_rep - 2)

    def make_and_send(peer):
        def one(slot, carry):
            sketch_head(
                peer * own_heads + slot, gram_stage.at[peer, slot], ch_stage.at[peer, slot]
            )
            gram_copy(peer, slot, me).start()
            ch_copy(peer, slot, me).start()
            return carry

        lax.fori_loop(0, own_heads, one, 0)

    def make_own(slot, carry):
        sketch_head(me * own_heads + slot, gram_in.at[me, slot], ch_in.at[me, slot])
        return carry

    others("seq", make_and_send)
    lax.fori_loop(0, own_heads, make_own, 0)

    def arrived(peer):
        for slot in range(own_heads):
            gram_copy(peer, slot, peer).wait_recv()
            ch_copy(peer, slot, peer).wait_recv()

    others("seq", arrived)

    diag = lax.broadcasted_iota(jnp.int32, (half, half), 0) == lax.broadcasted_iota(
        jnp.int32, (half, half), 1
    )
    ridge = jnp.where(diag, ridge_shift, 0.0)
    packs, chosen = [], []
    for slot in range(own_heads):
        total, picked = gram_in[0, slot], ch_in[0, slot].astype(jnp.float32)
        for source in range(1, n_seq):
            total = total + gram_in[source, slot]
            picked = picked + ch_in[source, slot].astype(jnp.float32)
        packs.append(total)
        chosen.append(picked)
    tokens = packs[0][half : half + 1, :1] + 1.0
    blocks = [
        (
            p[:half, :half] / tokens + ridge,
            p[:half, half:width] / tokens,
            p[:half, width:] / tokens + ridge,
        )
        for p in packs
    ]
    mine = pl.ds(pl.multiple_of(me * own_heads * width, width), own_heads * width)
    solved = solve_rows(blocks, chosen)
    solved_ref[:, mine] = jnp.concatenate(solved, axis=1).astype(jnp.bfloat16)

    def solved_copy(peer, source):
        span = pl.ds(pl.multiple_of(source * own_heads * width, width), own_heads * width)
        return peer_copy(
            solved_ref.at[:, span],
            solved_ref.at[:, span],
            solved_sems.at[0, peer],
            solved_sems.at[1, source],
            "seq",
            peer,
        )

    others("seq", lambda peer: solved_copy(peer, me).start())
    others("seq", lambda peer: solved_copy(peer, peer).wait_recv())
    score_ref[...] = lax.dot_general(
        sk_ref[...], solved_ref[...], NT, preferred_element_type=jnp.float32
    )

    def score_copy(peer, source):
        return peer_copy(
            score_ref.at[pl.ds(pl.multiple_of(peer * out_rows, out_rows), out_rows)],
            score_in.at[source],
            score_sems.at[0, peer],
            score_sems.at[1, source],
            "rep",
            peer,
        )

    own_rows = pl.ds(pl.multiple_of(layer * out_rows, out_rows), out_rows)
    others("rep", lambda peer: score_copy(peer, layer).start())
    score_in[layer] = score_ref[own_rows, :]
    others("rep", lambda peer: score_copy(peer, peer).wait_recv())
    contrib = score_in[0]
    for source in range(1, n_rep):
        contrib = contrib + score_in[source]

    def norm_copy(buf, sems, axis, peer, here, source):
        return peer_copy(
            buf.at[here], buf.at[source], sems.at[0, peer], sems.at[1, source], axis, peer
        )

    squares = jnp.sum(mask_ref[own_rows, :] * contrib * contrib, axis=0, keepdims=True)
    for buf, sems, axis, here, size in (
        (rep_norm, rep_sems, "rep", layer, n_rep),
        (seq_norm, seq_sems, "seq", me, n_seq),
    ):
        buf[here] = jnp.broadcast_to(squares, buf.shape[1:])
        others(axis, lambda peer: norm_copy(buf, sems, axis, peer, here, here).start())
        others(axis, lambda peer: norm_copy(buf, sems, axis, peer, here, peer).wait_recv())
        squares = buf[0, :1]
        for source in range(1, size):
            squares = squares + buf[source, :1]
    out_ref[...] = contrib / jnp.sqrt(squares / tokens + norm_floor)

    def sent(peer):
        for slot in range(own_heads):
            gram_copy(peer, slot, me).wait_send()
            ch_copy(peer, slot, me).wait_send()
        solved_copy(peer, me).wait_send()
        norm_copy(seq_norm, seq_sems, "seq", peer, me, me).wait_send()

    def sent_rep(peer):
        score_copy(peer, layer).wait_send()
        norm_copy(rep_norm, rep_sems, "rep", peer, layer, layer).wait_send()

    others("seq", sent)
    others("rep", sent_rep)


def on_device(head_out, grad_out, hash_codes, loss_mask, query_ids):
    outputs, gradient, codes = head_out[0], grad_out[0], hash_codes[0]
    n_seq, n_rep = lax.axis_size("seq"), lax.axis_size("rep")
    heads, depth = codes.shape
    rows, cols = outputs.shape
    width, own_heads = cols // heads, heads // n_seq
    queries = query_ids.shape[0]
    out_rows = rows // n_rep
    pack = (n_seq, own_heads, width // 2 + 8, width + width // 2)
    picked = (n_seq, own_heads, queries, width)
    vmem = pl.BlockSpec(memory_space=pltpu.VMEM)
    f32, bf16, dma = jnp.float32, jnp.bfloat16, pltpu.SemaphoreType.DMA
    return pl.pallas_call(
        functools.partial(whole_kernel, math.sqrt(width / depth), own_heads),
        in_specs=[vmem] * 5,
        out_specs=vmem,
        out_shape=jax.ShapeDtypeStruct((out_rows, queries), f32),
        scratch_shapes=[
            pltpu.VMEM((rows, cols), bf16),
            pltpu.VMEM((queries, rows), bf16),
            pltpu.VMEM(pack, f32),
            pltpu.VMEM(pack, f32),
            pltpu.VMEM(picked, bf16),
            pltpu.VMEM(picked, bf16),
            pltpu.VMEM((queries, cols), bf16),
            pltpu.VMEM((rows, queries), f32),
            pltpu.VMEM((n_rep, out_rows, queries), f32),
            pltpu.VMEM((n_rep, 8, queries), f32),
            pltpu.VMEM((n_seq, 8, queries), f32),
            dma((2, n_seq, own_heads)),
            dma((2, n_seq, own_heads)),
            dma((2, n_seq)),
            dma((2, n_rep)),
            dma((2, n_rep)),
            dma((2, n_seq)),
        ],
        compiler_params=pltpu.CompilerParams(
            collective_id=0, has_side_effects=True, vmem_limit_bytes=56 << 20
        ),
        name="attribute",
    )(
        gradient,
        outputs,
        codes,
        loss_mask.astype(f32)[:, None],
        query_ids[:, None],
    )


def solution(mesh):
    placed = (P("rep", "seq", None), P("rep", "seq", None), P("rep", None, None), P("seq"), P())
    return jax.shard_map(
        on_device, mesh=mesh, in_specs=placed, out_specs=P(("seq", "rep"), None), check_vma=False
    )
```

```python
import functools
import math

import jax
import jax.numpy as jnp
from jax import lax
from jax.experimental import pallas as pl
from jax.experimental.pallas import tpu as pltpu
from jax.sharding import PartitionSpec as P

ridge_shift = 0.25
norm_floor = 1e-06
NT = (((1,), (1,)), ((), ()))
TN = (((0,), (0,)), ((), ()))


def exact_dot(a, b, dims=(((1,), (0,)), ((), ()))):
    return lax.dot_general(
        a, b, dims, precision=lax.Precision.HIGHEST, preferred_element_type=jnp.float32
    )


def spd_inverse(mats):
    size = mats[0].shape[0]
    lane = lax.broadcasted_iota(jnp.int32, (1, size), 1)
    row8 = lax.broadcasted_iota(jnp.int32, (8, 1), 0)

    def pivots(_, mats):
        panels = [m[:8] for m in mats]
        for k in range(8):
            for i, p in enumerate(panels):
                row, col = p[k : k + 1, :], p[:, k : k + 1]
                inv = 1.0 / row[:, k : k + 1]
                scaled = jnp.where(lane == k, inv, row * inv)
                new = jnp.where(lane == k, 0.0, p) - col * scaled
                panels[i] = jnp.where(row8 == k, scaled, new)
        done = []
        for m, p in zip(mats, panels):
            rest = jnp.where(lane < 8, 0.0, m[8:]) - exact_dot(m[8:, :8], p)
            done.append(pltpu.roll(jnp.concatenate([rest, p], axis=0), size - 8, 1))
        return tuple(done)

    return lax.fori_loop(0, size // 8, pivots, tuple(mats))


def solve_rows(blocks, rows):
    half = blocks[0][0].shape[0]
    inv_a = spd_inverse([a for a, _, _ in blocks])
    w = [exact_dot(ia, b) for ia, (_, b, _) in zip(inv_a, blocks)]
    inv_s = spd_inverse([c - exact_dot(b, wi, TN) for (_, b, c), wi in zip(blocks, w)])
    out = []
    for r, ia, wi, si in zip(rows, inv_a, w, inv_s):
        second = exact_dot(r[:, half:] - exact_dot(r[:, :half], wi), si)
        first = exact_dot(r[:, :half], ia) - exact_dot(second, wi, NT)
        out.append(jnp.concatenate([first, second], axis=1))
    return out


def peer_copy(src, dst, send, recv, axis, index):
    return pltpu.make_async_remote_copy(
        src_ref=src,
        dst_ref=dst,
        send_sem=send,
        recv_sem=recv,
        device_id={axis: index},
        device_id_type=pl.DeviceIdType.MESH,
    )


def others(axis, body):
    size, me = lax.axis_size(axis), lax.axis_index(axis)

    def step(s, carry):
        body(lax.rem(me + 1 + s, size))
        return carry

    lax.fori_loop(0, size - 1, step, 0)


def whole_kernel(
    scale,
    own_heads,
    grad_ref,
    cols_ref,
    codes_ref,
    mask_ref,
    ids_ref,
    out_ref,
    sk_ref,
    hits_ref,
    gram_stage,
    gram_pair,
    gram_sum,
    gram_in,
    ch_stage,
    ch_pair,
    ch_sum,
    ch_in,
    solved_ref,
    score_ref,
    score_in,
    rep_norm,
    seq_norm,
    gram_pair_sems,
    ch_pair_sems,
    gram_sems,
    ch_sems,
    solved_sems,
    score_sems,
    rep_sems,
    seq_sems,
):
    n_seq, n_rep = lax.axis_size("seq"), lax.axis_size("rep")
    me, layer = lax.axis_index("seq"), lax.axis_index("rep")
    rows, depth = grad_ref.shape
    width = cols_ref.shape[1] // codes_ref.shape[0]
    half = width // 2
    out_rows = out_ref.shape[0]

    barrier = pltpu.get_barrier_semaphore()
    for axis in ("seq", "rep"):
        others(
            axis,
            lambda peer, axis=axis: pl.semaphore_signal(
                barrier, inc=1, device_id={axis: peer}, device_id_type=pl.DeviceIdType.MESH
            ),
        )

    mask = mask_ref[...]
    count = jnp.sum(mask, axis=0, keepdims=True)
    token = lax.broadcasted_iota(jnp.int32, (ids_ref.shape[0], rows), 1)
    hits_ref[...] = jnp.where(ids_ref[...] - me * rows == token, 1.0, 0.0).astype(jnp.bfloat16)

    def sketch_head(head, gram_to, ch_to):
        codes = codes_ref[pl.ds(head, 1), :]
        flipped = codes >= width
        bucket = jnp.where(flipped, codes - width, codes)
        bucket = bucket.astype(jnp.float32).astype(jnp.bfloat16)
        sign = jnp.where(flipped, -1.0, 1.0).astype(jnp.bfloat16)
        want = lax.broadcasted_iota(jnp.int32, (width, depth), 0)
        want = want.astype(jnp.float32).astype(jnp.bfloat16)
        table = jnp.where(bucket == want, sign, jnp.bfloat16(0))
        hashed = lax.dot_general(grad_ref[...], table, NT, preferred_element_type=jnp.float32)
        span = pl.ds(pl.multiple_of(head * width, width), width)
        sketch = (cols_ref[:, span].astype(jnp.float32) * hashed * scale).astype(jnp.bfloat16)
        sk_ref[:, span] = sketch
        gram = lax.dot_general(
            sketch * mask_ref[...].astype(jnp.bfloat16),
            sketch,
            TN,
            preferred_element_type=jnp.float32,
        )
        gram_to[:half, :width] = gram[:half]
        gram_to[:half, width:] = gram[half:, half:]
        gram_to[half:, :] = jnp.broadcast_to(count, (8, width + half))
        ch_to[...] = jnp.dot(
            hits_ref[...], sketch, preferred_element_type=jnp.float32
        ).astype(jnp.bfloat16)

    chips = n_seq // 2
    chip, side = me // 2, lax.rem(me, 2)
    partner = me + 1 - 2 * side

    def pair_copies(to, slot):
        return [
            peer_copy(
                src.at[to, slot],
                dst.at[to, slot],
                sems.at[0, to, slot],
                sems.at[1, to, slot],
                "seq",
                partner,
            )
            for src, dst, sems in (
                (gram_stage, gram_pair, gram_pair_sems),
                (ch_stage, ch_pair, ch_pair_sems),
            )
        ]

    def owner_copies(to, slot, source):
        return [
            peer_copy(
                src.at[to, slot],
                dst.at[source, slot],
                sems.at[0, to, slot],
                sems.at[1, source, slot],
                "seq",
                2 * to + side,
            )
            for src, dst, sems in ((gram_sum, gram_in, gram_sems), (ch_sum, ch_in, ch_sems))
        ]

    pl.semaphore_wait(barrier, n_seq + n_rep - 2)

    def for_partner(i, carry):
        to, slot = lax.rem(chip + 1 + i // own_heads, chips), lax.rem(i, own_heads)
        head = (2 * to + 1 - side) * own_heads + slot
        sketch_head(head, gram_stage.at[to, slot], ch_stage.at[to, slot])
        for copy in pair_copies(to, slot):
            copy.start()
        return carry

    def join(to, slot, gram_to, ch_to):
        sketch_head((2 * to + side) * own_heads + slot, gram_to, ch_to)
        for copy in pair_copies(to, slot):
            copy.wait_recv()
        gram_to[...] = gram_to[...] + gram_pair[to, slot]
        both = ch_to[...].astype(jnp.float32) + ch_pair[to, slot].astype(jnp.float32)
        ch_to[...] = both.astype(jnp.bfloat16)

    def for_owner(i, carry):
        to, slot = lax.rem(chip + 1 + i // own_heads, chips), lax.rem(i, own_heads)
        join(to, slot, gram_sum.at[to, slot], ch_sum.at[to, slot])
        for copy in owner_copies(to, slot, chip):
            copy.start()
        return carry

    def for_me(slot, carry):
        join(chip, slot, gram_in.at[chip, slot], ch_in.at[chip, slot])
        return carry

    def other_chips(body):
        def step(i, carry):
            to, slot = lax.rem(chip + 1 + i // own_heads, chips), lax.rem(i, own_heads)
            body(to, slot)
            return carry

        lax.fori_loop(0, (chips - 1) * own_heads, step, 0)

    def arrived(to, slot):
        for copy in owner_copies(to, slot, to):
            copy.wait_recv()

    lax.fori_loop(0, chips * own_heads, for_partner, 0)
    lax.fori_loop(0, (chips - 1) * own_heads, for_owner, 0)
    lax.fori_loop(0, own_heads, for_me, 0)
    other_chips(arrived)

    diag = lax.broadcasted_iota(jnp.int32, (half, half), 0) == lax.broadcasted_iota(
        jnp.int32, (half, half), 1
    )
    ridge = jnp.where(diag, ridge_shift, 0.0)
    packs, chosen = [], []
    for slot in range(own_heads):
        total, picked = gram_in[0, slot], ch_in[0, slot].astype(jnp.float32)
        for source in range(1, chips):
            total = total + gram_in[source, slot]
            picked = picked + ch_in[source, slot].astype(jnp.float32)
        packs.append(total)
        chosen.append(picked)
    tokens = packs[0][half : half + 1, :1] + 1.0
    blocks = [
        (
            p[:half, :half] / tokens + ridge,
            p[:half, half:width] / tokens,
            p[:half, width:] / tokens + ridge,
        )
        for p in packs
    ]
    mine = pl.ds(pl.multiple_of(me * own_heads * width, width), own_heads * width)
    solved = solve_rows(blocks, chosen)
    solved_ref[:, mine] = jnp.concatenate(solved, axis=1).astype(jnp.bfloat16)

    def solved_copy(peer, source):
        span = pl.ds(pl.multiple_of(source * own_heads * width, width), own_heads * width)
        return peer_copy(
            solved_ref.at[:, span],
            solved_ref.at[:, span],
            solved_sems.at[0, peer],
            solved_sems.at[1, source],
            "seq",
            peer,
        )

    others("seq", lambda peer: solved_copy(peer, me).start())
    others("seq", lambda peer: solved_copy(peer, peer).wait_recv())
    score_ref[...] = lax.dot_general(
        sk_ref[...], solved_ref[...], NT, preferred_element_type=jnp.float32
    )

    def score_copy(peer, source):
        return peer_copy(
            score_ref.at[pl.ds(pl.multiple_of(peer * out_rows, out_rows), out_rows)],
            score_in.at[source],
            score_sems.at[0, peer],
            score_sems.at[1, source],
            "rep",
            peer,
        )

    own_rows = pl.ds(pl.multiple_of(layer * out_rows, out_rows), out_rows)
    others("rep", lambda peer: score_copy(peer, layer).start())
    score_in[layer] = score_ref[own_rows, :]
    others("rep", lambda peer: score_copy(peer, peer).wait_recv())
    contrib = score_in[0]
    for source in range(1, n_rep):
        contrib = contrib + score_in[source]

    def norm_copy(buf, sems, axis, peer, here, source):
        return peer_copy(
            buf.at[here], buf.at[source], sems.at[0, peer], sems.at[1, source], axis, peer
        )

    squares = jnp.sum(mask_ref[own_rows, :] * contrib * contrib, axis=0, keepdims=True)
    for buf, sems, axis, here, size in (
        (rep_norm, rep_sems, "rep", layer, n_rep),
        (seq_norm, seq_sems, "seq", me, n_seq),
    ):
        buf[here] = jnp.broadcast_to(squares, buf.shape[1:])
        others(axis, lambda peer: norm_copy(buf, sems, axis, peer, here, here).start())
        others(axis, lambda peer: norm_copy(buf, sems, axis, peer, here, peer).wait_recv())
        squares = buf[0, :1]
        for source in range(1, size):
            squares = squares + buf[source, :1]
    out_ref[...] = contrib / jnp.sqrt(squares / tokens + norm_floor)

    def sent_pair(i, carry):
        for copy in pair_copies(i // own_heads, lax.rem(i, own_heads)):
            copy.wait_send()
        return carry

    def sent_owner(to, slot):
        for copy in owner_copies(to, slot, chip):
            copy.wait_send()

    def sent(peer):
        solved_copy(peer, me).wait_send()
        norm_copy(seq_norm, seq_sems, "seq", peer, me, me).wait_send()

    lax.fori_loop(0, chips * own_heads, sent_pair, 0)
    other_chips(sent_owner)

    def sent_rep(peer):
        score_copy(peer, layer).wait_send()
        norm_copy(rep_norm, rep_sems, "rep", peer, layer, layer).wait_send()

    others("seq", sent)
    others("rep", sent_rep)


def on_device(head_out, grad_out, hash_codes, loss_mask, query_ids):
    outputs, gradient, codes = head_out[0], grad_out[0], hash_codes[0]
    n_seq, n_rep = lax.axis_size("seq"), lax.axis_size("rep")
    heads, depth = codes.shape
    rows, cols = outputs.shape
    width, own_heads = cols // heads, heads // n_seq
    queries = query_ids.shape[0]
    out_rows = rows // n_rep
    pack = (n_seq // 2, own_heads, width // 2 + 8, width + width // 2)
    picked = (n_seq // 2, own_heads, queries, width)
    vmem = pl.BlockSpec(memory_space=pltpu.VMEM)
    f32, bf16, dma = jnp.float32, jnp.bfloat16, pltpu.SemaphoreType.DMA
    return pl.pallas_call(
        functools.partial(whole_kernel, math.sqrt(width / depth), own_heads),
        in_specs=[vmem] * 5,
        out_specs=vmem,
        out_shape=jax.ShapeDtypeStruct((out_rows, queries), f32),
        scratch_shapes=[
            pltpu.VMEM((rows, cols), bf16),
            pltpu.VMEM((queries, rows), bf16),
            *[pltpu.VMEM(pack, f32)] * 4,
            *[pltpu.VMEM(picked, bf16)] * 4,
            pltpu.VMEM((queries, cols), bf16),
            pltpu.VMEM((rows, queries), f32),
            pltpu.VMEM((n_rep, out_rows, queries), f32),
            pltpu.VMEM((n_rep, 8, queries), f32),
            pltpu.VMEM((n_seq, 8, queries), f32),
            *[dma((2, n_seq // 2, own_heads))] * 4,
            dma((2, n_seq)),
            dma((2, n_rep)),
            dma((2, n_rep)),
            dma((2, n_seq)),
        ],
        compiler_params=pltpu.CompilerParams(
            collective_id=0, has_side_effects=True, vmem_limit_bytes=56 << 20
        ),
        name="attribute",
    )(
        gradient,
        outputs,
        codes,
        loss_mask.astype(f32)[:, None],
        query_ids[:, None],
    )


def solution(mesh):
    placed = (P("rep", "seq", None), P("rep", "seq", None), P("rep", None, None), P("seq"), P())
    return jax.shard_map(
        on_device, mesh=mesh, in_specs=placed, out_specs=P(("seq", "rep"), None), check_vma=False
    )
```

```python
import functools
import math

import jax
import jax.numpy as jnp
from jax import lax
from jax.experimental import pallas as pl
from jax.experimental.pallas import tpu as pltpu
from jax.sharding import PartitionSpec as P

ridge_shift = 0.25
norm_floor = 1e-06
NT = (((1,), (1,)), ((), ()))
TN = (((0,), (0,)), ((), ()))


def exact_dot(a, b, dims=(((1,), (0,)), ((), ()))):
    return lax.dot_general(
        a, b, dims, precision=lax.Precision.HIGHEST, preferred_element_type=jnp.float32
    )


def spd_inverse(mats):
    size = mats[0].shape[0]
    lane = lax.broadcasted_iota(jnp.int32, (1, size), 1)
    row8 = lax.broadcasted_iota(jnp.int32, (8, 1), 0)

    def pivots(_, mats):
        panels = [m[:8] for m in mats]
        for k in range(8):
            for i, p in enumerate(panels):
                row, col = p[k : k + 1, :], p[:, k : k + 1]
                inv = 1.0 / row[:, k : k + 1]
                scaled = jnp.where(lane == k, inv, row * inv)
                new = jnp.where(lane == k, 0.0, p) - col * scaled
                panels[i] = jnp.where(row8 == k, scaled, new)
        done = []
        for m, p in zip(mats, panels):
            rest = jnp.where(lane < 8, 0.0, m[8:]) - exact_dot(m[8:, :8], p)
            done.append(pltpu.roll(jnp.concatenate([rest, p], axis=0), size - 8, 1))
        return tuple(done)

    return lax.fori_loop(0, size // 8, pivots, tuple(mats))


def solve_rows(blocks, rows):
    half = blocks[0][0].shape[0]
    inv_a = spd_inverse([a for a, _, _ in blocks])
    w = [exact_dot(ia, b) for ia, (_, b, _) in zip(inv_a, blocks)]
    inv_s = spd_inverse([c - exact_dot(b, wi, TN) for (_, b, c), wi in zip(blocks, w)])
    out = []
    for r, ia, wi, si in zip(rows, inv_a, w, inv_s):
        second = exact_dot(r[:, half:] - exact_dot(r[:, :half], wi), si)
        first = exact_dot(r[:, :half], ia) - exact_dot(second, wi, NT)
        out.append(jnp.concatenate([first, second], axis=1))
    return out


def peer_copy(src, dst, send, recv, axis, index):
    return pltpu.make_async_remote_copy(
        src_ref=src,
        dst_ref=dst,
        send_sem=send,
        recv_sem=recv,
        device_id={axis: index},
        device_id_type=pl.DeviceIdType.MESH,
    )


def others(axis, body):
    size, me = lax.axis_size(axis), lax.axis_index(axis)

    def step(s, carry):
        body(lax.rem(me + 1 + s, size))
        return carry

    lax.fori_loop(0, size - 1, step, 0)


def whole_kernel(
    scale,
    own_heads,
    grad_ref,
    cols_ref,
    codes_ref,
    mask_row_ref,
    ids_ref,
    out_ref,
    mask_ref,
    sk_ref,
    hits_ref,
    gram_stage,
    gram_pair,
    gram_sum,
    gram_in,
    ch_stage,
    ch_pair,
    ch_sum,
    ch_in,
    solved_ref,
    score_ref,
    score_in,
    rep_norm,
    seq_norm,
    gram_pair_sems,
    ch_pair_sems,
    gram_sems,
    ch_sems,
    solved_sems,
    score_sems,
    rep_sems,
    seq_sems,
):
    n_seq, n_rep = lax.axis_size("seq"), lax.axis_size("rep")
    me, layer = lax.axis_index("seq"), lax.axis_index("rep")
    rows, depth = grad_ref.shape
    width = cols_ref.shape[1] // codes_ref.shape[0]
    half = width // 2
    out_rows = out_ref.shape[0]

    barrier = pltpu.get_barrier_semaphore()
    for axis in ("seq", "rep"):
        others(
            axis,
            lambda peer, axis=axis: pl.semaphore_signal(
                barrier, inc=1, device_id={axis: peer}, device_id_type=pl.DeviceIdType.MESH
            ),
        )

    mask = mask_row_ref[...].astype(jnp.float32)
    count = jnp.sum(mask, axis=1, keepdims=True)
    mask_ref[...] = jnp.transpose(jnp.broadcast_to(mask, (128, rows)))[:, :1]
    token = lax.broadcasted_iota(jnp.int32, (rows, ids_ref.shape[1]), 0)
    hits_ref[...] = jnp.where(ids_ref[...] - me * rows == token, 1.0, 0.0).astype(jnp.bfloat16)

    def sketch_head(head, gram_to, ch_to):
        codes = codes_ref[pl.ds(head, 1), :]
        flipped = codes >= width
        bucket = jnp.where(flipped, codes - width, codes)
        bucket = bucket.astype(jnp.float32).astype(jnp.bfloat16)
        sign = jnp.where(flipped, -1.0, 1.0).astype(jnp.bfloat16)
        want = lax.broadcasted_iota(jnp.int32, (width, depth), 0)
        want = want.astype(jnp.float32).astype(jnp.bfloat16)
        table = jnp.where(bucket == want, sign, jnp.bfloat16(0))
        hashed = lax.dot_general(grad_ref[...], table, NT, preferred_element_type=jnp.float32)
        span = pl.ds(pl.multiple_of(head * width, width), width)
        sketch = (cols_ref[:, span].astype(jnp.float32) * hashed * scale).astype(jnp.bfloat16)
        sk_ref[:, span] = sketch
        gram = lax.dot_general(
            sketch * mask_ref[...].astype(jnp.bfloat16),
            sketch,
            TN,
            preferred_element_type=jnp.float32,
        )
        gram_to[:half, :width] = gram[:half]
        gram_to[:half, width:] = gram[half:, half:]
        gram_to[half:, :] = jnp.broadcast_to(count, (8, width + half))
        ch_to[...] = lax.dot_general(
            hits_ref[...], sketch, TN, preferred_element_type=jnp.float32
        ).astype(jnp.bfloat16)

    chips = n_seq // 2
    chip, side = me // 2, lax.rem(me, 2)
    partner = me + 1 - 2 * side

    def pair_copies(to, slot):
        return [
            peer_copy(
                src.at[to, slot],
                dst.at[to, slot],
                sems.at[0, to, slot],
                sems.at[1, to, slot],
                "seq",
                partner,
            )
            for src, dst, sems in (
                (gram_stage, gram_pair, gram_pair_sems),
                (ch_stage, ch_pair, ch_pair_sems),
            )
        ]

    def owner_copies(to, slot, source):
        return [
            peer_copy(
                src.at[to, slot],
                dst.at[source, slot],
                sems.at[0, to, slot],
                sems.at[1, source, slot],
                "seq",
                2 * to + side,
            )
            for src, dst, sems in ((gram_sum, gram_in, gram_sems), (ch_sum, ch_in, ch_sems))
        ]

    pl.semaphore_wait(barrier, n_seq + n_rep - 2)

    def for_partner(i, carry):
        to, slot = lax.rem(chip + 1 + i // own_heads, chips), lax.rem(i, own_heads)
        head = (2 * to + 1 - side) * own_heads + slot
        sketch_head(head, gram_stage.at[to, slot], ch_stage.at[to, slot])
        for copy in pair_copies(to, slot):
            copy.start()
        return carry

    def join(to, slot, gram_to, ch_to):
        sketch_head((2 * to + side) * own_heads + slot, gram_to, ch_to)
        for copy in pair_copies(to, slot):
            copy.wait_recv()
        gram_to[...] = gram_to[...] + gram_pair[to, slot]
        both = ch_to[...].astype(jnp.float32) + ch_pair[to, slot].astype(jnp.float32)
        ch_to[...] = both.astype(jnp.bfloat16)

    def for_owner(i, carry):
        to, slot = lax.rem(chip + 1 + i // own_heads, chips), lax.rem(i, own_heads)
        join(to, slot, gram_sum.at[to, slot], ch_sum.at[to, slot])
        for copy in owner_copies(to, slot, chip):
            copy.start()
        return carry

    def for_me(slot, carry):
        join(chip, slot, gram_in.at[chip, slot], ch_in.at[chip, slot])
        return carry

    def other_chips(body):
        def step(i, carry):
            to, slot = lax.rem(chip + 1 + i // own_heads, chips), lax.rem(i, own_heads)
            body(to, slot)
            return carry

        lax.fori_loop(0, (chips - 1) * own_heads, step, 0)

    def arrived(to, slot):
        for copy in owner_copies(to, slot, to):
            copy.wait_recv()

    lax.fori_loop(0, chips * own_heads, for_partner, 0)
    lax.fori_loop(0, (chips - 1) * own_heads, for_owner, 0)
    lax.fori_loop(0, own_heads, for_me, 0)
    other_chips(arrived)

    diag = lax.broadcasted_iota(jnp.int32, (half, half), 0) == lax.broadcasted_iota(
        jnp.int32, (half, half), 1
    )
    ridge = jnp.where(diag, ridge_shift, 0.0)
    packs, chosen = [], []
    for slot in range(own_heads):
        total, picked = gram_in[0, slot], ch_in[0, slot].astype(jnp.float32)
        for source in range(1, chips):
            total = total + gram_in[source, slot]
            picked = picked + ch_in[source, slot].astype(jnp.float32)
        packs.append(total)
        chosen.append(picked)
    tokens = packs[0][half : half + 1, :1] + 1.0
    blocks = [
        (
            p[:half, :half] / tokens + ridge,
            p[:half, half:width] / tokens,
            p[:half, width:] / tokens + ridge,
        )
        for p in packs
    ]
    mine = pl.ds(pl.multiple_of(me * own_heads * width, width), own_heads * width)
    solved = solve_rows(blocks, chosen)
    solved_ref[:, mine] = jnp.concatenate(solved, axis=1).astype(jnp.bfloat16)

    def solved_copy(peer, source):
        span = pl.ds(pl.multiple_of(source * own_heads * width, width), own_heads * width)
        return peer_copy(
            solved_ref.at[:, span],
            solved_ref.at[:, span],
            solved_sems.at[0, peer],
            solved_sems.at[1, source],
            "seq",
            peer,
        )

    others("seq", lambda peer: solved_copy(peer, me).start())
    others("seq", lambda peer: solved_copy(peer, peer).wait_recv())
    score_ref[...] = lax.dot_general(
        sk_ref[...], solved_ref[...], NT, preferred_element_type=jnp.float32
    )

    def score_copy(peer, source):
        return peer_copy(
            score_ref.at[pl.ds(pl.multiple_of(peer * out_rows, out_rows), out_rows)],
            score_in.at[source],
            score_sems.at[0, peer],
            score_sems.at[1, source],
            "rep",
            peer,
        )

    own_rows = pl.ds(pl.multiple_of(layer * out_rows, out_rows), out_rows)
    others("rep", lambda peer: score_copy(peer, layer).start())
    score_in[layer] = score_ref[own_rows, :]
    others("rep", lambda peer: score_copy(peer, peer).wait_recv())
    contrib = score_in[0]
    for source in range(1, n_rep):
        contrib = contrib + score_in[source]

    def norm_copy(buf, sems, axis, peer, here, source):
        return peer_copy(
            buf.at[here], buf.at[source], sems.at[0, peer], sems.at[1, source], axis, peer
        )

    squares = jnp.sum(mask_ref[own_rows, :] * contrib * contrib, axis=0, keepdims=True)
    for buf, sems, axis, here, size in (
        (rep_norm, rep_sems, "rep", layer, n_rep),
        (seq_norm, seq_sems, "seq", me, n_seq),
    ):
        buf[here] = jnp.broadcast_to(squares, buf.shape[1:])
        others(axis, lambda peer: norm_copy(buf, sems, axis, peer, here, here).start())
        others(axis, lambda peer: norm_copy(buf, sems, axis, peer, here, peer).wait_recv())
        squares = buf[0, :1]
        for source in range(1, size):
            squares = squares + buf[source, :1]
    out_ref[...] = contrib / jnp.sqrt(squares / tokens + norm_floor)

    def sent_pair(i, carry):
        for copy in pair_copies(i // own_heads, lax.rem(i, own_heads)):
            copy.wait_send()
        return carry

    def sent_owner(to, slot):
        for copy in owner_copies(to, slot, chip):
            copy.wait_send()

    def sent(peer):
        solved_copy(peer, me).wait_send()
        norm_copy(seq_norm, seq_sems, "seq", peer, me, me).wait_send()

    lax.fori_loop(0, chips * own_heads, sent_pair, 0)
    other_chips(sent_owner)

    def sent_rep(peer):
        score_copy(peer, layer).wait_send()
        norm_copy(rep_norm, rep_sems, "rep", peer, layer, layer).wait_send()

    others("seq", sent)
    others("rep", sent_rep)


def on_device(head_out, grad_out, hash_codes, loss_mask, query_ids):
    outputs, gradient, codes = head_out[0], grad_out[0], hash_codes[0]
    n_seq, n_rep = lax.axis_size("seq"), lax.axis_size("rep")
    heads, depth = codes.shape
    rows, cols = outputs.shape
    width, own_heads = cols // heads, heads // n_seq
    queries = query_ids.shape[0]
    out_rows = rows // n_rep
    pack = (n_seq // 2, own_heads, width // 2 + 8, width + width // 2)
    picked = (n_seq // 2, own_heads, queries, width)
    vmem = pl.BlockSpec(memory_space=pltpu.VMEM)
    f32, bf16, dma = jnp.float32, jnp.bfloat16, pltpu.SemaphoreType.DMA
    return pl.pallas_call(
        functools.partial(whole_kernel, math.sqrt(width / depth), own_heads),
        in_specs=[vmem] * 5,
        out_specs=vmem,
        out_shape=jax.ShapeDtypeStruct((out_rows, queries), f32),
        scratch_shapes=[
            pltpu.VMEM((rows, 1), f32),
            pltpu.VMEM((rows, cols), bf16),
            pltpu.VMEM((rows, queries), bf16),
            *[pltpu.VMEM(pack, f32)] * 4,
            *[pltpu.VMEM(picked, bf16)] * 4,
            pltpu.VMEM((queries, cols), bf16),
            pltpu.VMEM((rows, queries), f32),
            pltpu.VMEM((n_rep, out_rows, queries), f32),
            pltpu.VMEM((n_rep, 8, queries), f32),
            pltpu.VMEM((n_seq, 8, queries), f32),
            *[dma((2, n_seq // 2, own_heads))] * 4,
            dma((2, n_seq)),
            dma((2, n_rep)),
            dma((2, n_rep)),
            dma((2, n_seq)),
        ],
        compiler_params=pltpu.CompilerParams(
            collective_id=0, has_side_effects=True, vmem_limit_bytes=56 << 20
        ),
        name="attribute",
    )(
        gradient,
        outputs,
        codes,
        loss_mask[None, :],
        query_ids[None, :],
    )


def solution(mesh):
    placed = (P("rep", "seq", None), P("rep", "seq", None), P("rep", None, None), P("seq"), P())
    return jax.shard_map(
        on_device, mesh=mesh, in_specs=placed, out_specs=P(("seq", "rep"), None), check_vma=False
    )
```
